32 devices in a mesh: dp: 4 (over y, z), tp: 8 (over x, core).
Axes of the slice: x: 4, y: 2, z: 2, core: 2. Of those that a mesh axis runs over, the one named last changes fastest.
The devices are a block of a 4x4x8 slice.
Arguments:
- x: bfloat16 [1024, 2048], P(('dp', 'tp')), parts along dimension 0
- grad_y: bfloat16 [1024, 2048], P(('dp', 'tp')), parts along dimension 0
- gain_attn: float32 [2, 2048], replicated
- gain_mlp: float32 [2, 2048], replicated
- w_qkv: bfloat16 [2, 2048, 6144], P(None, None, 'tp')
- w_out: bfloat16 [2, 2048, 2048], P(None, 'tp')
- w_gate: bfloat16 [2, 2048, 8192], P(None, None, 'tp')
- w_up: bfloat16 [2, 2048, 8192], P(None, None, 'tp')
- w_down: bfloat16 [2, 8192, 2048], P(None, 'tp')
Outputs:
- output 1: bfloat16 [1024, 2048], P(('dp', 'tp')), parts along dimension 0
- output 2: bfloat16 [1024, 2048], P(('dp', 'tp')), parts along dimension 0
- output 3: bfloat16 [8, 2048, 6144], P('dp', None, 'tp'), parts along dimension 0
- output 4: bfloat16 [8, 2048, 2048], P('dp', 'tp'), parts along dimension 0
- output 5: bfloat16 [8, 2048, 8192], P('dp', None, 'tp'), parts along dimension 0
- output 6: bfloat16 [8, 2048, 8192], P('dp', None, 'tp'), parts along dimension 0
- output 7: bfloat16 [8, 8192, 2048], P('dp', 'tp'), parts along dimension 0
- output 8: float32 [8, 2048], P('dp'), parts along dimension 0
- output 9: float32 [8, 2048], P('dp'), parts along dimension 0
There are 4 independent parts. The reference program is written for one: setup_inputs(seed, part) draws one part's arguments, and reference() takes and returns one part's arrays. A program takes and returns all parts, laid end to end along the dimension named above; an argument that names none is the same for every part.
All inputs are finite; a program needn't handle non-finite values.
Results may differ from the reference program's by a relative error of at most 0.017051.
Values are sent between devices in bfloat16 or wider.
A program may use at most 768 MiB of HBM per device.

```python
import jax
import jax.numpy as jnp
from jax import lax

D = 2048
FF = 8192
HEADS = 16
KV_HEADS = 16
HEAD = 128
LAYERS = 2
SEQ_LEN = 256
NORM_EPS = 1e-5
GROUP_SIZE = HEADS // KV_HEADS
QKV_COLS = (HEADS + 2 * KV_HEADS) * HEAD


def setup_inputs(seed: int = 0, part: int = 0) -> dict:
    part_key = jax.random.fold_in(jax.random.key(seed), part)
    act_keys = jax.random.split(part_key, 4)
    weight_keys = jax.random.split(jax.random.key(seed + 1), 7)
    x_mean = jax.random.normal(act_keys[0], (1, D), jnp.float32)
    x = jax.random.normal(act_keys[1], (SEQ_LEN, D), jnp.float32) + x_mean
    grad_mean = jax.random.normal(act_keys[2], (1, D), jnp.float32)
    grad_y = jax.random.normal(act_keys[3], (SEQ_LEN, D), jnp.float32) + grad_mean
    gain_attn = 1.0 + 0.3 * jax.random.normal(weight_keys[0], (LAYERS, D), jnp.float32)
    gain_mlp = 1.0 + 0.3 * jax.random.normal(weight_keys[1], (LAYERS, D), jnp.float32)
    w_qkv = jax.random.normal(weight_keys[2], (LAYERS, D, QKV_COLS), jnp.float32) * D ** -0.5
    w_out = jax.random.normal(weight_keys[3], (LAYERS, HEADS * HEAD, D), jnp.float32) * (HEADS * HEAD) ** -0.5
    w_gate = jax.random.normal(weight_keys[4], (LAYERS, D, FF), jnp.float32) * D ** -0.5
    w_up = jax.random.normal(weight_keys[5], (LAYERS, D, FF), jnp.float32) * D ** -0.5
    w_down = jax.random.normal(weight_keys[6], (LAYERS, FF, D), jnp.float32) * FF ** -0.5
    return {'x': x.astype(jnp.bfloat16), 'grad_y': grad_y.astype(jnp.bfloat16), 'gain_attn': gain_attn, 'gain_mlp': gain_mlp, 'w_qkv': w_qkv.astype(jnp.bfloat16), 'w_out': w_out.astype(jnp.bfloat16), 'w_gate': w_gate.astype(jnp.bfloat16), 'w_up': w_up.astype(jnp.bfloat16), 'w_down': w_down.astype(jnp.bfloat16)}


def rms_norm(hidden_in, gain_vec):
    hidden_f = hidden_in.astype(jnp.float32)
    inv_rms = lax.rsqrt(jnp.mean(hidden_f * hidden_f, axis=-1, keepdims=True) + NORM_EPS)
    return (hidden_f * inv_rms * gain_vec).astype(jnp.bfloat16)


def attention(qkv_out):
    positions = jnp.arange(SEQ_LEN)
    causal = positions[:, None] >= positions[None, :]

    def one_group(group_block):
        queries = group_block[:, :GROUP_SIZE].astype(jnp.float32)
        key_rows = group_block[:, GROUP_SIZE].astype(jnp.float32)
        value_rows = group_block[:, GROUP_SIZE + 1].astype(jnp.float32)
        scores = jnp.einsum('iqh,jh->qij', queries, key_rows) * HEAD ** -0.5
        prob_low = jax.nn.softmax(jnp.where(causal, scores, -1e30), axis=-1).astype(jnp.bfloat16)
        heads_out = jnp.einsum('qij,jh->iqh', prob_low.astype(jnp.float32), value_rows)
        return heads_out.astype(jnp.bfloat16)

    blocks = jnp.moveaxis(qkv_out.reshape(SEQ_LEN, KV_HEADS, GROUP_SIZE + 2, HEAD), 1, 0)
    heads_out = lax.map(jax.checkpoint(one_group), blocks)
    return jnp.moveaxis(heads_out, 0, 1).reshape(SEQ_LEN, HEADS * HEAD)


def decoder_layer(hidden_in, params):
    gain_attn, gain_mlp, w_qkv, w_out, w_gate, w_up, w_down = params
    normed = rms_norm(hidden_in, gain_attn)
    qkv_out = jnp.dot(normed, w_qkv, preferred_element_type=jnp.float32).astype(jnp.bfloat16)
    heads_out = attention(qkv_out)
    hidden_mid = hidden_in + jnp.dot(heads_out, w_out, preferred_element_type=jnp.float32).astype(jnp.bfloat16)
    normed_mid = rms_norm(hidden_mid, gain_mlp)
    gate_act = jnp.dot(normed_mid, w_gate, preferred_element_type=jnp.float32).astype(jnp.bfloat16)
    up_act = jnp.dot(normed_mid, w_up, preferred_element_type=jnp.float32).astype(jnp.bfloat16)
    gated_act = (jax.nn.silu(gate_act.astype(jnp.float32)) * up_act.astype(jnp.float32)).astype(jnp.bfloat16)
    return hidden_mid + jnp.dot(gated_act, w_down, preferred_element_type=jnp.float32).astype(jnp.bfloat16)


def stack_forward(x, params):
    def scan_body(hidden_carry, layer_params):
        return decoder_layer(hidden_carry, layer_params), None
    hidden_out, _ = lax.scan(scan_body, x, params)
    return hidden_out


def reference(x, grad_y, gain_attn, gain_mlp, w_qkv, w_out, w_gate, w_up, w_down):
    params = (gain_attn, gain_mlp, w_qkv, w_out, w_gate, w_up, w_down)
    y, pullback = jax.vjp(stack_forward, x, params)
    grad_x, grad_params = pullback(grad_y)
    return (y, grad_x, grad_params[2], grad_params[3], grad_params[4], grad_params[5], grad_params[6], grad_params[0], grad_params[1])
```

```python
import functools

import jax
import jax.numpy as jnp
from jax import lax
from jax.experimental import pallas as pl
from jax.experimental.pallas import tpu as pltpu
from jax.sharding import PartitionSpec as P

HEAD_DIM = 128
NORM_EPS = 1e-5
BF = jnp.bfloat16
F32 = jnp.float32
CHUNKS = 4
VMEM_LIMIT = 62 * 1024 * 1024


def dot_nn(a, b):
    return lax.dot_general(a, b, (((1,), (0,)), ((), ())), preferred_element_type=F32)


def dot_nt(a, b):
    return lax.dot_general(a, b, (((1,), (1,)), ((), ())), preferred_element_type=F32)


def dot_tn(a, b):
    return lax.dot_general(a, b, (((0,), (0,)), ((), ())), preferred_element_type=F32)


def norm(h, gain):
    hf = h.astype(F32)
    inv = lax.rsqrt(jnp.mean(hf * hf, axis=-1, keepdims=True) + NORM_EPS)
    return (hf * inv * gain).astype(BF)


def norm_grad(h, gain, dy):
    hf = h.astype(F32)
    dyf = dy.astype(F32)
    inv = lax.rsqrt(jnp.mean(hf * hf, axis=-1, keepdims=True) + NORM_EPS)
    hn = hf * inv
    dgain = jnp.sum(dyf * hn, axis=0, keepdims=True)
    gdy = dyf * gain
    dh = inv * (gdy - hn * jnp.mean(gdy * hn, axis=-1, keepdims=True))
    return dh.astype(BF), dgain


class Place:
    def __init__(self, n):
        self.n = n
        self.me = lax.axis_index('tp')
        self.side = lax.rem(self.me, 2)
        self.chip = self.me // 2
        nc = n // 2
        self.lchip = lax.rem(self.chip + nc - 1, nc)
        self.rchip = lax.rem(self.chip + 1, nc)
        self.ochip = lax.rem(self.chip + 2, nc)
        self.partner = self.chip * 2 + 1 - self.side
        self.left = self.lchip * 2 + self.side
        self.right = self.rchip * 2 + self.side
        self.opp = self.ochip * 2 + self.side
        self.pleft = self.lchip * 2 + 1 - self.side
        self.pright = self.rchip * 2 + 1 - self.side
        self.popp = self.ochip * 2 + 1 - self.side

    def barrier(self, everyone=False):
        sem = pltpu.get_barrier_semaphore()
        if everyone:
            for k in range(1, self.n):
                pl.semaphore_signal(sem, inc=1, device_id={'tp': lax.rem(self.me + k, self.n)},
                                    device_id_type=pl.DeviceIdType.MESH)
            pl.semaphore_wait(sem, self.n - 1)
        else:
            for peer in (self.partner, self.left, self.right):
                pl.semaphore_signal(sem, inc=1, device_id={'tp': peer}, device_id_type=pl.DeviceIdType.MESH)
            pl.semaphore_wait(sem, 3)


def remote(src, dst, ssem, rsem, peer):
    return pltpu.make_async_remote_copy(src_ref=src, dst_ref=dst, send_sem=ssem, recv_sem=rsem,
                                        device_id={'tp': peer}, device_id_type=pl.DeviceIdType.MESH)


class Gather:
    def __init__(self, place, buf, ssem, rsem):
        self.p, self.buf, self.ssem, self.rsem = place, buf, ssem, rsem
        self.rows = buf.shape[0] // place.n
        self.half = self.rows // 2
        self.sent = []

    def view(self, shard, part):
        if part is None:
            return self.buf.at[pl.ds(pl.multiple_of(shard * self.rows, self.rows), self.rows), :]
        return self.buf.at[pl.ds(pl.multiple_of(shard * self.rows + part * self.half, self.half), self.half), :]

    def send(self, k, peer, shard, part):
        v = self.view(shard, part)
        cp = remote(v, v, self.ssem.at[k], self.rsem.at[k], peer)
        cp.start()
        self.sent.append(cp)

    def recv(self, k, shard, part):
        v = self.view(shard, part)
        remote(v, v, self.ssem.at[k], self.rsem.at[k], self.p.partner).wait_recv()

    def start(self):
        p = self.p
        self.send(1, p.right, p.me, 0)
        self.send(3, p.left, p.me, 1)
        self.send(2, p.right, p.me, 1)
        self.send(4, p.left, p.me, 0)
        self.send(0, p.partner, p.me, None)

    def finish(self):
        p = self.p
        self.recv(1, p.left, 0)
        self.send(5, p.right, p.left, 0)
        self.send(7, p.partner, p.left, 0)
        self.recv(3, p.right, 1)
        self.send(6, p.left, p.right, 1)
        self.send(8, p.partner, p.right, 1)
        self.recv(2, p.left, 1)
        self.send(9, p.partner, p.left, 1)
        self.recv(4, p.right, 0)
        self.send(10, p.partner, p.right, 0)
        self.recv(5, p.opp, 0)
        self.send(11, p.partner, p.opp, 0)
        self.recv(6, p.opp, 1)
        self.send(12, p.partner, p.opp, 1)
        self.recv(0, p.partner, None)
        self.recv(7, p.pleft, 0)
        self.recv(8, p.pright, 1)
        self.recv(9, p.pleft, 1)
        self.recv(10, p.pright, 0)
        self.recv(11, p.popp, 0)
        self.recv(12, p.popp, 1)
        for cp in self.sent:
            cp.wait_send()
        self.sent = []


class Scatter:
    def __init__(self, place, part, pair, froml, fromr, dsem, rsem):
        self.p = place
        self.part, self.pair, self.froml, self.fromr = part, pair, froml, fromr
        self.dsem, self.rsem = dsem, rsem
        self.rows, self.cols = part.shape[3], part.shape[4]
        self.half = self.rows // 2

    def pair_copy(self, c):
        return remote(self.part.at[c, :, 1 - self.p.side], self.pair.at[c], self.dsem.at[0, c], self.dsem.at[1, c],
                      self.p.partner)

    def ring_copy(self, c, to_right, kind, chip, part):
        src = self.pair.at[c, chip, pl.ds(part * self.half, self.half), :]
        dst = (self.froml if to_right else self.fromr).at[c, kind]
        d = 0 if to_right else 1
        return remote(src, dst, self.rsem.at[0, d, kind, c], self.rsem.at[1, d, kind, c],
                      self.p.right if to_right else self.p.left)

    def run(self, compute, out, filler=None):
        p, half = self.p, self.half
        nchip = self.part.shape[1]
        sent = []

        def start(cp):
            cp.start()
            sent.append(cp)

        def produce(c):
            self.part[c] = compute(c).reshape(nchip, 2, self.rows, self.cols)
            start(self.pair_copy(c))

        def first(c):
            self.pair_copy(c).wait_recv()
            for chip in (p.ochip, p.rchip, p.lchip):
                self.pair[c, chip] = self.pair[c, chip] + self.part[c, chip, p.side]
                if chip is p.ochip:
                    start(self.ring_copy(c, True, 0, chip, 0))
                    start(self.ring_copy(c, False, 0, chip, 1))
                elif chip is p.rchip:
                    start(self.ring_copy(c, True, 1, chip, 1))
                else:
                    start(self.ring_copy(c, False, 1, chip, 0))

        def second(c):
            lo, hi = pl.ds(0, half), pl.ds(half, half)
            self.ring_copy(c, True, 0, p.ochip, 0).wait_recv()
            self.pair[c, p.rchip, lo, :] = self.pair[c, p.rchip, lo, :] + self.froml[c, 0]
            start(self.ring_copy(c, True, 2, p.rchip, 0))
            self.ring_copy(c, False, 0, p.ochip, 1).wait_recv()
            self.pair[c, p.lchip, hi, :] = self.pair[c, p.lchip, hi, :] + self.fromr[c, 0]
            start(self.ring_copy(c, False, 2, p.lchip, 1))

        def last(c):
            own = self.pair[c, p.chip] + self.part[c, p.chip, p.side]
            for d in (True, False):
                for kind in (1, 2):
                    self.ring_copy(c, d, kind, p.chip, 0).wait_recv()
            cs = pl.ds(c * self.cols, self.cols)
            out[0:half, cs] = own[0:half] + self.froml[c, 2] + self.fromr[c, 1]
            out[half:2 * half, cs] = own[half:2 * half] + self.froml[c, 1] + self.fromr[c, 2]

        for t in range(CHUNKS + 1):
            if t < CHUNKS:
                produce(t)
            if t >= 1:
                first(t - 1)
        if filler is not None:
            filler()
        for c in range(CHUNKS):
            second(c)
        for c in range(CHUNKS):
            last(c)
        for cp in sent:
            cp.wait_send()


def cols_loop(total, step, body):
    def one(i, carry):
        body(pl.multiple_of(i * step, step))
        return carry
    lax.fori_loop(0, total // step, one, 0)


def attention_forward(qkv, heads, o, prob=None):
    seq = qkv.shape[0]
    rows = lax.broadcasted_iota(jnp.int32, (seq, seq), 0)
    cols = lax.broadcasted_iota(jnp.int32, (seq, seq), 1)
    causal = rows >= cols
    for h in range(heads):
        at = h * 3 * HEAD_DIM
        q, k, v = (qkv[:, at + j * HEAD_DIM:at + (j + 1) * HEAD_DIM] for j in range(3))
        s = jnp.where(causal, dot_nt(q, k) * HEAD_DIM ** -0.5, -1e30)
        e = jnp.exp(s - jnp.max(s, axis=-1, keepdims=True))
        pr = e / jnp.sum(e, axis=-1, keepdims=True)
        if prob is not None:
            prob[h] = pr
        o[:, h * HEAD_DIM:(h + 1) * HEAD_DIM] = dot_nn(pr.astype(BF), v).astype(BF)


def attention_backward(qkv, heads, prob, d_heads, d_qkv):
    for h in range(heads):
        at = h * 3 * HEAD_DIM
        q, k, v = (qkv[:, at + j * HEAD_DIM:at + (j + 1) * HEAD_DIM] for j in range(3))
        do = d_heads[:, h * HEAD_DIM:(h + 1) * HEAD_DIM]
        pr = prob[h]
        dp = dot_nt(do, v)
        dv = dot_tn(pr.astype(BF), do)
        ds = (pr * (dp - jnp.sum(dp * pr, axis=-1, keepdims=True)) * HEAD_DIM ** -0.5).astype(BF)
        d_qkv[:, at:at + HEAD_DIM] = dot_nn(ds, k).astype(BF)
        d_qkv[:, at + HEAD_DIM:at + 2 * HEAD_DIM] = dot_tn(ds, q).astype(BF)
        d_qkv[:, at + 2 * HEAD_DIM:at + 3 * HEAD_DIM] = dv.astype(BF)


def sigmoid(x):
    return 1.0 / (1.0 + jnp.exp(-x))


def forward_kernel(n, layers, x, gain_a, gain_m, wq_h, wo_h, wg_h, wu_h, wd_h,
                   y, *rest):
    kept = rest[:layers - 1]
    (wq, wo, wg, wu, wd, ubuf, nbuf, qkv, o, mact, part, pair, froml, fromr, acc,
     wsem, us, ur, ns, nr, dsem, rsem) = rest[layers - 1:]
    place = Place(n)
    loads = []
    for l in range(layers):
        loads.append([])
        for j, (src, dst) in enumerate(((wq_h, wq), (wo_h, wo), (wg_h, wg), (wu_h, wu), (wd_h, wd))):
            cp = pltpu.make_async_copy(src.at[l], dst.at[l], wsem.at[l, j])
            cp.start()
            loads[l].append(cp)
    place.barrier()
    rows = x.shape[0]
    mine = pl.ds(pl.multiple_of(place.me * rows, rows), rows)
    heads = qkv.shape[1] // (3 * HEAD_DIM)
    scatter = Scatter(place, part, pair, froml, fromr, dsem, rsem)
    h = x[...]
    cc = part.shape[4]
    for l in range(layers):
        ubuf[mine, :] = norm(h, gain_a[l:l + 1, :])
        gather = Gather(place, ubuf, us, ur)
        gather.start()
        gather.finish()
        loads[l][0].wait()

        def qkv_cols(at):
            qkv[:, pl.ds(at, 256)] = dot_nn(ubuf[...], wq[l, :, pl.ds(at, 256)]).astype(BF)
        cols_loop(qkv.shape[1], 256, qkv_cols)
        attention_forward(qkv, heads, o)
        loads[l][1].wait()
        scatter.run(lambda c: dot_nn(o[...], wo[l, :, c * cc:(c + 1) * cc]), acc)
        h1 = h + acc[...].astype(BF)
        nbuf[mine, :] = norm(h1, gain_m[l:l + 1, :])
        gather = Gather(place, nbuf, ns, nr)
        gather.start()
        loads[l][2].wait()
        loads[l][3].wait()
        gather.finish()

        def mlp_cols(at):
            cs = pl.ds(at, 256)
            z1 = dot_nn(nbuf[...], wg[l, :, cs]).astype(BF).astype(F32)
            z3 = dot_nn(nbuf[...], wu[l, :, cs]).astype(BF).astype(F32)
            mact[:, cs] = (z1 * sigmoid(z1) * z3).astype(BF)
        cols_loop(mact.shape[1], 256, mlp_cols)
        loads[l][4].wait()
        scatter.run(lambda c: dot_nn(mact[...], wd[l, :, c * cc:(c + 1) * cc]), acc)
        h = h1 + acc[...].astype(BF)
        if l < layers - 1:
            kept[l][...] = h
    y[...] = h


def backward_kernel(n, l, others, share, hin, dout, gain_a, gain_m, wq_h, wo_h, wg_h, wu_h, wd_h, *rest):
    gains_in = None
    if others:
        gains_in, rest = rest[0], rest[1:]
    (dx, gains, u_h, n_h, do_h, da_h, o_h, m_h, dg_h, du_h, dqkv_h,
     wq, wo, wg, wu, wd, ubuf, nbuf, dobuf, dabuf, qkv, o, prob, mact, dgate, dup, dgated, dheads, dqkv,
     part, pair, froml, fromr, acc,
     wsem, osem, us, ur, ns, nr, dos, dor, das, dar, dsem, rsem, gs, gr) = rest
    place = Place(n)
    loads = []
    for j, (src, dst) in enumerate(((wq_h, wq), (wo_h, wo), (wd_h, wd), (wg_h, wg), (wu_h, wu))):
        cp = pltpu.make_async_copy(src.at[l], dst, wsem.at[j])
        cp.start()
        loads.append(cp)
    place.barrier(everyone=share)
    stores = []

    def store(src, dst):
        cp = pltpu.make_async_copy(src, dst, osem.at[len(stores)])
        cp.start()
        stores.append(cp)

    rows = hin.shape[0]
    mine = pl.ds(pl.multiple_of(place.me * rows, rows), rows)
    heads = qkv.shape[1] // (3 * HEAD_DIM)
    scatter = Scatter(place, part, pair, froml, fromr, dsem, rsem)
    cc = part.shape[4]
    ga, gm = gain_a[l:l + 1, :], gain_m[l:l + 1, :]

    h = hin[...]
    ubuf[mine, :] = norm(h, ga)
    gu = Gather(place, ubuf, us, ur)
    gu.start()
    dobuf[mine, :] = dout[...]
    gd = Gather(place, dobuf, dos, dor)
    gd.start()
    gu.finish()
    loads[0].wait()

    def qkv_cols(at):
        qkv[:, pl.ds(at, 256)] = dot_nn(ubuf[...], wq[:, pl.ds(at, 256)]).astype(BF)
    cols_loop(qkv.shape[1], 256, qkv_cols)
    attention_forward(qkv, heads, o, prob)
    gd.finish()
    store(ubuf, u_h)
    store(o, o_h)
    store(dobuf, do_h)
    loads[1].wait()
    loads[2].wait()

    def gated_cols():
        def body(at):
            dgated[:, pl.ds(at, 256)] = dot_nt(dobuf[...], wd[pl.ds(at, 256), :])
        cols_loop(dgated.shape[1], 256, body)
    scatter.run(lambda c: dot_nn(o[...], wo[:, c * cc:(c + 1) * cc]), acc, gated_cols)
    h1 = h + acc[...].astype(BF)
    nbuf[mine, :] = norm(h1, gm)
    gn = Gather(place, nbuf, ns, nr)
    gn.start()
    loads[3].wait()
    loads[4].wait()
    gn.finish()
    store(nbuf, n_h)

    def mlp_cols(at):
        cs = pl.ds(at, 256)
        z1 = dot_nn(nbuf[...], wg[:, cs]).astype(BF).astype(F32)
        z3 = dot_nn(nbuf[...], wu[:, cs]).astype(BF).astype(F32)
        sg = sigmoid(z1)
        act = z1 * sg
        mact[:, cs] = (act * z3).astype(BF)
        dm = dgated[:, cs].astype(BF).astype(F32)
        dup[:, cs] = (dm * act).astype(BF)
        dgate[:, cs] = (dm * z3 * (sg * (1.0 + z1 * (1.0 - sg)))).astype(BF)
    cols_loop(mact.shape[1], 256, mlp_cols)
    store(mact, m_h)
    store(dgate, dg_h)
    store(dup, du_h)

    scatter.run(lambda c: dot_nt(dgate[...], wg[c * cc:(c + 1) * cc, :]) + dot_nt(dup[...], wu[c * cc:(c + 1) * cc, :]), acc)
    d_norm, dgain_m = norm_grad(h1, gm, acc[...].astype(BF))
    d_h1 = dout[...] + d_norm
    dabuf[mine, :] = d_h1
    gda = Gather(place, dabuf, das, dar)
    gda.start()
    gda.finish()
    store(dabuf, da_h)

    def heads_cols(at):
        dheads[:, pl.ds(at, 128)] = dot_nt(dabuf[...], wo[pl.ds(at, 128), :]).astype(BF)
    cols_loop(dheads.shape[1], 128, heads_cols)
    attention_backward(qkv, heads, prob, dheads, dqkv)
    store(dqkv, dqkv_h)
    scatter.run(lambda c: dot_nt(dqkv[...], wq[c * cc:(c + 1) * cc, :]), acc)
    d_norm, dgain_a = norm_grad(h, ga, acc[...].astype(BF))
    dx[...] = d_h1 + d_norm
    if share:
        me = place.me
        if others:
            gains[me, 2:, :] = gains_in[...]
        gains[me, 0:1, :] = dgain_a
        gains[me, 1:2, :] = dgain_m
        cps = []
        for k in range(1, n):
            cp = remote(gains.at[me], gains.at[me], gs.at[k], gr.at[k], lax.rem(me + k, n))
            cp.start()
            cps.append(cp)
        for k in range(1, n):
            src = lax.rem(me + n - k, n)
            remote(gains.at[src], gains.at[src], gs.at[k], gr.at[k], place.partner).wait_recv()
        for cp in cps:
            cp.wait_send()
    else:
        k = 0
        if others:
            gains[2:, :] = gains_in[...]
        gains[0:1, :] = dgain_a
        gains[1:2, :] = dgain_m
    for cp in stores:
        cp.wait()


def weight_kernel(last, *refs):
    refs = list(refs)
    u, nn, do, da, o, m, dg, du, dqkv = refs[:9]
    refs = refs[9:]
    if last:
        y, dx, gains = refs[:3]
        refs = refs[3 + 5:]
        gq, go, gg, gu, gd, y_o, dx_o, ga_o, gm_o = refs
    else:
        gq, go, gg, gu, gd = refs
    gq[0] = dot_tn(u[...], dqkv[...]).astype(BF)
    go[0] = dot_tn(o[...], da[...]).astype(BF)
    gg[0] = dot_tn(nn[...], dg[...]).astype(BF)
    gu[0] = dot_tn(nn[...], du[...]).astype(BF)
    gd[0] = dot_tn(m[...], do[...]).astype(BF)
    if last:
        @pl.when(pl.program_id(0) == 0)
        def _():
            y_o[...] = y[...]
            dx_o[...] = dx[...]
            total = gains[0]
            for k in range(1, gains.shape[0]):
                total = total + gains[k]
            for j in range(ga_o.shape[0]):
                ga_o[j:j + 1, :] = total[2 * j:2 * j + 1, :]
                gm_o[j:j + 1, :] = total[2 * j + 1:2 * j + 2, :]


def solution(mesh):
    n = mesh.shape['tp']
    row_spec = P(('dp', 'tp'), None)
    col_spec = P(None, None, 'tp')
    mid_spec = P(None, 'tp', None)
    in_specs = (row_spec, row_spec, P(None, None), P(None, None), col_spec, mid_spec, col_spec, col_spec, mid_spec)
    out_specs = (row_spec, row_spec, P('dp', None, 'tp'), P('dp', 'tp', None), P('dp', None, 'tp'), P('dp', None, 'tp'), P('dp', 'tp', None), P('dp', None), P('dp', None))
    vm = pl.BlockSpec(memory_space=pltpu.VMEM)
    hbm = pl.BlockSpec(memory_space=pl.ANY)
    DMA = pltpu.SemaphoreType.DMA

    def step(x, grad_y, gain_attn, gain_mlp, w_qkv, w_out, w_gate, w_up, w_down):
        layers, d, qcols = w_qkv.shape
        ocols = w_out.shape[1]
        ff = w_gate.shape[2]
        rows = x.shape[0]
        seq = rows * n
        heads = qcols // (3 * HEAD_DIM)
        cc = d // CHUNKS
        nchip = n // 2
        weights = (w_qkv, w_out, w_gate, w_up, w_down)
        shard = jax.ShapeDtypeStruct((rows, d), BF)

        def comm_scratch():
            return [
                pltpu.VMEM((CHUNKS, nchip, 2, rows, cc), F32),
                pltpu.VMEM((CHUNKS, nchip, rows, cc), F32),
                pltpu.VMEM((CHUNKS, 3, rows // 2, cc), F32),
                pltpu.VMEM((CHUNKS, 3, rows // 2, cc), F32),
                pltpu.VMEM((rows, d), F32),
            ]

        def wscratch(*lead):
            return [pltpu.VMEM((*lead, *w.shape[1:]), BF) for w in weights]

        full = pltpu.VMEM((seq, d), BF)
        fwd = pl.pallas_call(
            functools.partial(forward_kernel, n, layers),
            out_shape=[shard] * layers,
            in_specs=[vm] * 3 + [hbm] * 5,
            out_specs=[vm] * layers,
            scratch_shapes=wscratch(layers) + [full, full, pltpu.VMEM((seq, qcols), BF), pltpu.VMEM((seq, ocols), BF),
                                               pltpu.VMEM((seq, ff), BF)] + comm_scratch()
            + [DMA((layers, 5))] + [DMA((13,))] * 4 + [DMA((2, CHUNKS)), DMA((2, 2, 3, CHUNKS))],
            compiler_params=pltpu.CompilerParams(collective_id=0, has_side_effects=True, vmem_limit_bytes=VMEM_LIMIT),
            name='fwd',
        )(x, gain_attn, gain_mlp, *weights)
        y = fwd[0]
        layer_in = [x] + list(fwd[1:])
        d_hidden = grad_y
        grads = None
        gains = None
        gshapes = [jax.ShapeDtypeStruct(w.shape, BF) for w in weights]
        for l in reversed(range(layers)):
            done = layers - 1 - l
            share = l == 0
            gshape = (2 * (done + 1), d)
            res = [((seq, d), BF)] * 4 + [((seq, ocols), BF)] + [((seq, ff), BF)] * 3 + [((seq, qcols), BF)]
            gsem = [DMA((n,)), DMA((n,))]
            out = pl.pallas_call(
                functools.partial(backward_kernel, n, l, done > 0, share),
                out_shape=[shard, jax.ShapeDtypeStruct(((n,) if share else ()) + gshape, F32)]
                + [jax.ShapeDtypeStruct(s, t) for s, t in res],
                in_specs=[vm] * 4 + [hbm] * 5 + ([vm] if done else []),
                out_specs=[vm] * 2 + [hbm] * 9,
                scratch_shapes=wscratch() + [full] * 4 + [
                    pltpu.VMEM((seq, qcols), BF), pltpu.VMEM((seq, ocols), BF), pltpu.VMEM((heads, seq, seq), F32),
                    pltpu.VMEM((seq, ff), BF), pltpu.VMEM((seq, ff), BF), pltpu.VMEM((seq, ff), BF),
                    pltpu.VMEM((seq, ff), F32), pltpu.VMEM((seq, ocols), BF), pltpu.VMEM((seq, qcols), BF),
                ] + comm_scratch() + [DMA((5,)), DMA((9,))] + [DMA((13,))] * 8
                + [DMA((2, CHUNKS)), DMA((2, 2, 3, CHUNKS))] + gsem,
                compiler_params=pltpu.CompilerParams(collective_id=1 + done, has_side_effects=True,
                                                     vmem_limit_bytes=VMEM_LIMIT),
                name=f'bwd{l}',
            )(layer_in[l], d_hidden, gain_attn, gain_mlp, *weights, *([gains] if done else []))
            d_hidden, gains = out[0], out[1]
            u, nn, do, da, o, m, dg, du, dqkv = out[2:]
            steps = d // 256
            ins = [
                (u, pl.BlockSpec((seq, 256), lambda i: (0, i))),
                (nn, pl.BlockSpec((seq, 256), lambda i: (0, i))),
                (do, pl.BlockSpec((seq, d), lambda i: (0, 0))),
                (da, pl.BlockSpec((seq, 256), lambda i: (0, i))),
                (o, pl.BlockSpec((seq, ocols), lambda i: (0, 0))),
                (m, pl.BlockSpec((seq, ff // steps), lambda i: (0, i))),
                (dg, pl.BlockSpec((seq, ff), lambda i: (0, 0))),
                (du, pl.BlockSpec((seq, ff), lambda i: (0, 0))),
                (dqkv, pl.BlockSpec((seq, qcols), lambda i: (0, 0))),
            ]
            outs = [
                pl.BlockSpec((1, 256, qcols), lambda i, l=l: (l, i, 0)),
                pl.BlockSpec((1, ocols, 256), lambda i, l=l: (l, 0, i)),
                pl.BlockSpec((1, 256, ff), lambda i, l=l: (l, i, 0)),
                pl.BlockSpec((1, 256, ff), lambda i, l=l: (l, i, 0)),
                pl.BlockSpec((1, ff // steps, d), lambda i, l=l: (l, i, 0)),
            ]
            oshape = list(gshapes)
            alias = {}
            whole = lambda a: pl.BlockSpec(a.shape, lambda i: (0,) * len(a.shape))
            if share:
                ins += [(a, whole(a)) for a in (y, d_hidden, gains)]
                gsum = jax.ShapeDtypeStruct((layers, d), F32)
                oshape += [shard, shard, gsum, gsum]
                outs += [whole(s) for s in (shard, shard, gsum, gsum)]
            if grads is not None:
                alias = {len(ins) + j: j for j in range(5)}
                ins += [(g, hbm) for g in grads]
            grads = pl.pallas_call(
                functools.partial(weight_kernel, share),
                grid=(steps,),
                out_shape=oshape,
                in_specs=[s for _, s in ins],
                out_specs=outs,
                input_output_aliases=alias,
                compiler_params=pltpu.CompilerParams(dimension_semantics=('arbitrary',)),
                name=f'wgrad{l}',
            )(*[a for a, _ in ins])
        gq, go, gg, gu, gd, y, d_hidden, gsa, gsm = grads
        return (y, d_hidden, gq, go, gg, gu, gd, gsa, gsm)

    return jax.shard_map(step, mesh=mesh, in_specs=in_specs, out_specs=out_specs, check_vma=False)
```
